256 devices in a mesh: wide: 16 (over z, y_hi), narrow: 8 (over x, y_lo), grp: 2 (over core).
Axes of the slice: x: 4, y: 4 (y_hi: 2, y_lo: 2; y = y_hi * 2 + y_lo), z: 8, core: 2. Of those that a mesh axis runs over, the one named last changes fastest.
Arguments:
- boundary_block: float32 [16, 1024, 16384], P(None, ('narrow', 'grp'), 'wide'), may hold values from -4 to 4
- schur_blocks: float32 [8, 1536, 1536], P('narrow', ('wide', 'grp')), may hold values from -2 to 2
- interface_rows: int32 [8, 1536], P('narrow'), may hold values from 0 to 2047, as said below
- live_rows: int32 [8], P('narrow'), may hold values from 1 to 1536, 9216 in all
- row_scale: float32 [16, 1024], P('wide', ('narrow', 'grp')), may hold values from 0.4 to 1.2
- excitation: float32 [16, 1024, 128], P('wide', ('narrow', 'grp')), may hold values from -6 to 6
Outputs:
- traces: float32 [16, 1024, 128], P('wide', ('narrow', 'grp'))
- residual: float32 [16, 1024, 128], P('wide', ('narrow', 'grp'))
The draws below stay inside these ranges and needn't reach their ends.
Inputs may be any that keep to these rules, and one draw needn't show every extreme that they name: `interface_rows`: each substructure's row holds 1536 different positions, 0 to 2047; within each aligned block of 48 slots, at most 2 positions lie in one aligned range of 64 positions, and every substructure reaches 2 in some block.
All inputs are finite; a program needn't handle non-finite values. No bound on the sum of `live_rows` on one device may be relied on, other than what follows from the above.
Results may differ from the reference program's by a relative error of at most 0.00016.
Values sent between devices are 32-bit elements; how exact they have to be, the bound alone decides.
A program may use at most 64 MiB of HBM per device.

```python
import math
import jax
import jax.numpy as jnp
import numpy as np
from jax import lax

NB = 16384
M = 1536
SUB_PAN = 1
R = 128
ITERS = 3
NSUB = 8
PANEL = 2048
N_WIDE = 16
N_NARROW = 8
N_GRP = 2


def draw_boundary_block(key, part):
    spread = jax.random.normal(key, (NB, NB), jnp.float32)
    matrix = jnp.eye(NB, dtype=jnp.float32) + spread * (0.5 / NB ** 0.5)
    return matrix.T.reshape(N_WIDE, NB // N_WIDE, NB)


def draw_schur_blocks(key, part):
    spread = jax.random.normal(key, (NSUB, M, M), jnp.float32)
    return 0.25 * jnp.eye(M, dtype=jnp.float32)[None] + spread * (0.12 / M ** 0.5)


def draw_interface_rows(key, part):
    blocks = N_WIDE * N_GRP
    piece = PANEL // blocks
    keys = jax.random.split(jax.random.fold_in(key, 7), NSUB)
    places = jnp.arange(PANEL, dtype=jnp.int32)
    counter = jnp.arange(M, dtype=jnp.int32)
    slot_of = counter % blocks * (M // blocks) + counter // blocks

    def one(single):
        first, second = jax.random.split(single)
        ranks = jax.random.permutation(first, PANEL).astype(jnp.int32)
        whole_owner = jax.random.randint(second, (), 0, blocks, dtype=jnp.int32)
        scores = ranks - jnp.where(places // piece == whole_owner, PANEL, 0).astype(jnp.int32)
        chosen = jnp.argsort(scores, stable=True)[:M].astype(jnp.int32)
        by_owner = chosen[jnp.argsort(chosen // piece, stable=True)]
        return jnp.zeros((M,), jnp.int32).at[slot_of].set(by_owner)
    return jax.vmap(one)(keys).astype(jnp.int32)


def block_levels(own_key, extent, pieces, least, high):
    level, own = 1.0, jax.random.fold_in(own_key, 6)
    for axis_at, parts in pieces:
        steps = jnp.exp(jax.random.uniform(jax.random.fold_in(own, axis_at), (parts,), jnp.float32, least / len(pieces), high / len(pieces)))
        level = level * jnp.repeat(steps, extent[axis_at] // parts).reshape([-1 if axis == axis_at else 1 for axis in range(len(extent))])
    return level


def profile(number_of, total, limit, skew):
    portions = [(1 << 20) // math.isqrt(standing ** skew) + 1 for standing in range(2, number_of + 1)]
    spare, given = total - limit - (number_of - 1), [1] * (number_of - 1)
    while spare > 0:
        candidates = [i for i in range(number_of - 1) if given[i] < limit]
        pool, left = sum([portions[i] for i in candidates]), spare
        for i in candidates:
            more = min(limit - given[i], max(1, left * portions[i] // pool), spare)
            given[i] = given[i] + more
            spare = spare - more
    return np.array([limit] + given)


def ragged_sizes(own_key, count, total, bound, lean):
    if count == 2:
        one = jax.random.randint(own_key, (), max(1, total - bound), min(bound, total - 1) + 1)
        return jnp.stack([one, total - one])
    tallies = jnp.asarray(profile(count, total, bound, lean), jnp.int32)
    twos = (count - 1) // 2
    source_of, sink = tallies[1:1 + 2 * twos:2], tallies[2:2 + 2 * twos:2]
    room = jnp.minimum(source_of - 1, bound - sink)
    shifted = jax.random.randint(jax.random.fold_in(own_key, 1), (twos,), 0, 1 << 20) % (room + 1)
    tallies = tallies.at[1:1 + 2 * twos:2].set(source_of - shifted).at[2:2 + 2 * twos:2].set(sink + shifted)
    return tallies[jax.random.permutation(jax.random.fold_in(own_key, 2), count)]


def normal_values(key, shape, deviation, most, shards=(), kind=jnp.bfloat16):
    entries = jax.random.normal(key, shape, jnp.float32) * deviation
    if len(shards) > 0:
        entries = block_levels(key, shape, shards, -0.22, 0.18) * entries
    return jnp.clip(entries, min=-most, max=most).astype(kind)


def setup_inputs(seed: int = 0) -> dict:
    key_list = jax.random.split(jax.random.key(seed), 7)
    return {
        "boundary_block": draw_boundary_block(jax.random.fold_in(key_list[6], 71), 0),
        "schur_blocks": draw_schur_blocks(jax.random.fold_in(key_list[6], 71), 0),
        "interface_rows": draw_interface_rows(jax.random.fold_in(key_list[6], 71), 0),
        "live_rows": ragged_sizes(key_list[3], NSUB, NSUB * M * 3 // 4, M, 2).astype(jnp.int32),
        "row_scale": jnp.clip(jnp.exp(math.log(1.2) - 1.0986123 * jax.random.uniform(key_list[4], (N_WIDE, NB // N_WIDE), jnp.float32) ** block_levels(key_list[4], (N_WIDE, NB // N_WIDE), ((0, 16), (1, 16)), -0.2, 0.2)), 0.4, 1.2),
        "excitation": normal_values(key_list[5], (N_WIDE, NB // N_WIDE, R), 1.0, 6.0, ((0, 16), (1, 16)), jnp.float32),
    }


RELAX = 0.35


def reference(boundary_block, schur_blocks, interface_rows, live_rows, row_scale, excitation):
    column_major = boundary_block.reshape(NB, NB)
    row_weight = row_scale.reshape(NB, 1)
    forcing = excitation.reshape(NB, R)
    strip_width = NB // (N_WIDE * N_NARROW)
    panel_index = jnp.arange(NSUB, dtype=jnp.int32) // SUB_PAN
    global_rows = ((interface_rows // strip_width) * (NB // N_WIDE) + panel_index[:, None] * strip_width + interface_rows % strip_width).astype(jnp.int32)
    positions = jnp.arange(M, dtype=jnp.int32)
    live_mask = (positions[None, :] < live_rows[:, None]).astype(jnp.float32)

    def operate(current):
        boundary = lax.dot_general(column_major, current, (((0,), (0,)), ((), ())), precision=lax.Precision.HIGHEST, preferred_element_type=jnp.float32)

        def add_one(totals, inputs):
            schur, targets, weights = inputs
            local = current[targets] * weights[:, None]
            result = jnp.dot(schur, local, precision=lax.Precision.HIGHEST, preferred_element_type=jnp.float32) * weights[:, None]
            return totals.at[targets].add(result), None

        interface, unused = lax.scan(add_one, jnp.zeros((NB, R), jnp.float32), (schur_blocks, global_rows, live_mask))
        return boundary + interface

    traces = RELAX * row_weight * forcing
    residual = forcing
    for sweep in range(ITERS):
        residual = forcing - operate(traces)
        traces = traces + RELAX * row_weight * residual
    return traces.reshape(N_WIDE, NB // N_WIDE, R), residual.reshape(N_WIDE, NB // N_WIDE, R)
```

```python
import functools

import jax
import jax.numpy as jnp
from jax import lax
from jax.experimental import pallas as pl
from jax.experimental.pallas import tpu as pltpu
from jax.sharding import PartitionSpec as P

ITERS = 3
RELAX = 0.35
MESH = pl.DeviceIdType.MESH
NZ, NX = 8, 4

SLOTS = [
    (0, 0), (0, 1), (1, 0), (1, 1), (7, 0), (7, 1), (2, 0), (2, 1),
    (6, 0), (6, 1), (3, 0), (3, 1), (5, 0), (5, 1), (4, 0), (4, 1),
]
SLOT_OF = {v: i for i, v in enumerate(SLOTS)}
PARENT = {v: ((0, 0) if v[1] == 0 or v[0] == 0 else (v[0], 0)) for v in SLOTS if v != (0, 0)}
ROOT_ORDER = [(1, 0), (7, 0), (2, 0), (6, 0), (3, 0), (5, 0), (4, 0), (0, 1)]
PLAN = [
    (1, 0), (7, 0), (2, 0), (6, 0), (3, 0), (5, 0), (4, 0), (0, 1), (1, 1), 0,
    (7, 1), (2, 1), 1, (6, 1), (3, 1), 2, (5, 1), (4, 1), 3,
]
PAIRS = [(dx, dy) for dx in (2, 1, 3, 0) for dy in (1, 0) if (dx, dy) != (0, 0)]
FAR = [
    (dz, dy, dg)
    for dz in (4, 3, 5, 2, 6, 1, 7, 0)
    for dy in (1, 0)
    for dg in (1, 0)
    if (dz, dy, dg) != (0, 0, 0)
]


def halves(value):
    high = value.astype(jnp.bfloat16)
    low = (value - high.astype(jnp.float32)).astype(jnp.bfloat16)
    return high, low


def dot(a, b):
    return jnp.dot(a, b, preferred_element_type=jnp.float32)


def dot_t(a, b):
    return lax.dot_general(a, b, (((1,), (1,)), ((), ())), preferred_element_type=jnp.float32)


def kernel(
    bb, schur, q_row, q_blocks, live, scale, exc, out_t, out_r,
    bload, sboth, lhs_h, lhs_l, gath, part, from_core, to_pair, from_pair, to_far, from_far,
    keys, place, weight,
    load_sem, s_send, s_recv, g_send, g_recv, c_send, c_recv, p_send, p_recv, f_send, f_recv,
):
    wide, narrow, grp = lax.axis_index("wide"), lax.axis_index("narrow"), lax.axis_index("grp")
    z, yh, x, yl = wide // 2, wide % 2, narrow // 2, narrow % 2
    share = sboth.shape[1]
    iface = sboth.shape[2]
    extra = 2 * share

    def wide_at(dz, dy):
        return ((z + dz) % NZ) * 2 + (yh + dy) % 2

    def narrow_at(dx, dy):
        return ((x + dx) % NX) * 2 + (yl + dy) % 2

    def remote(src, dst, send, recv, device):
        return pltpu.make_async_remote_copy(
            src_ref=src, dst_ref=dst, send_sem=send, recv_sem=recv, device_id=device, device_id_type=MESH
        )

    barrier = pltpu.get_barrier_semaphore()
    for dz, dy, dg in FAR:
        pl.semaphore_signal(
            barrier, inc=1, device_id=(wide_at(dz, dy), narrow, (grp + dg) % 2), device_id_type=MESH
        )
    for dx, dy in PAIRS:
        pl.semaphore_signal(barrier, inc=1, device_id=(wide, narrow_at(dx, dy), grp), device_id_type=MESH)

    s_load = pltpu.make_async_copy(schur.at[0], sboth.at[grp], load_sem.at[16])
    s_load.start()
    b_loads = []
    for i, (dz, dy) in enumerate(SLOTS):
        source = ((z + NZ - dz) % NZ) * 2 + (yh + dy) % 2
        b_loads.append(pltpu.make_async_copy(bb.at[source], bload.at[i], load_sem.at[i]))
        b_loads[-1].start()

    forcing = exc[0]
    own = jnp.broadcast_to(scale[...], (64, 64))
    diagonal = lax.broadcasted_iota(jnp.int32, (64, 64), 0) == lax.broadcasted_iota(jnp.int32, (64, 64), 1)
    column = jnp.sum(jnp.where(diagonal, own, 0.0), axis=1, keepdims=True)
    weight[...] = jnp.broadcast_to(RELAX * column, (64, 128))
    gath[0, 0] = weight[...] * forcing
    live_count = live[0]

    pl.semaphore_wait(barrier, len(FAR) + len(PAIRS))

    def gather_copy(it, v):
        parent = PARENT[v]
        device = (wide_at(v[0] - parent[0], v[1] - parent[1] + 2), narrow, grp)
        k = SLOT_OF[v]
        return remote(
            gath.at[it, SLOT_OF[parent]], gath.at[it, k], g_send.at[it, k - 1], g_recv.at[it, k - 1], device
        )

    def hand_on(it, v):
        order = ROOT_ORDER if v == (0, 0) else SLOTS[1:]
        for child in order:
            if PARENT[child] == v:
                gather_copy(it, child).start()

    hand_on(0, (0, 0))
    s_load.wait()
    s_copy = remote(sboth.at[grp], sboth.at[grp], s_send, s_recv, (wide, narrow, 1 - grp))
    s_copy.start()

    def split_block(c):
        for i in range(4 * c, 4 * c + 4):
            b_loads[i].wait()
        for h in range(2):
            i = 4 * c + 2 * h
            block = bload[i : i + 2].reshape(128, bload.shape[2])
            for m in range(0, block.shape[1], 256):
                high, low = halves(block[:, m : m + 256].T)
                lhs_h[c, pl.ds(extra + m, 256), pl.ds(128 * h, 128)] = high
                lhs_l[c, pl.ds(extra + m, 256), pl.ds(128 * h, 128)] = low

    def split_schur(c):
        q = q_row[...]
        lane = lax.broadcasted_iota(jnp.int32, (1, iface), 1)
        q = jnp.where(lane < live_count, q, -1)
        rows = []
        for i in range(4 * c, 4 * c + 4):
            dz, dy = SLOTS[i]
            source = ((z + NZ - dz) % NZ) * 2 + (yh + dy) % 2
            shifted = jnp.broadcast_to(q - (source * 128 + grp * 64), (64, iface))
            hit = shifted == lax.broadcasted_iota(jnp.int32, (64, iface), 0)
            rows.append(jnp.where(hit, 1.0, 0.0).astype(jnp.bfloat16))
        picked = jnp.concatenate(rows, axis=0)
        high, low = halves(sboth[...].reshape(extra, iface))
        lhs_h[c, 0:extra, :] = dot_t(high, picked).astype(jnp.bfloat16)
        lhs_l[c, 0:extra, :] = dot_t(low, picked).astype(jnp.bfloat16)

    def index_tables():
        q = q_blocks[...]
        blocks = q.shape[0]
        lane = lax.broadcasted_iota(jnp.int32, (blocks, 128), 1)
        block = lax.broadcasted_iota(jnp.int32, (blocks, 128), 0)
        owner = q // 64
        rank = jnp.zeros_like(q)
        for d in range(1, share):
            same = (pltpu.roll(owner, d, 1) == owner) & (lane >= d)
            rank = rank + jnp.where(same, 1, 0)
        used = (lane < share) & (block * share + lane < live_count)
        core = block % 2
        keys[...] = jnp.where(used, owner * 4 + core * 2 + rank, -1)
        mine = used & (owner == wide * 2 + grp)
        rowpos = jnp.zeros((1, 128), jnp.int32)
        for level in range(2):
            spot = jnp.where(mine & (rank == level), q % 64 + 1, 0)
            spot = jnp.sum(spot, axis=1, keepdims=True)
            match = (block == 2 * (lane // 8) + (lane % 4) // 2) & (lane % 2 == level)
            rowpos = rowpos + jnp.sum(jnp.where(match, spot, 0), axis=0, keepdims=True)
        row = lax.broadcasted_iota(jnp.int32, (64, 128), 0)
        place[...] = jnp.where(row == rowpos - 1, 1.0, 0.0).astype(jnp.bfloat16)

    def multiply(it, c):
        high, low = halves(gath[it, 4 * c : 4 * c + 4].reshape(256, 128))
        both = jnp.concatenate([high, low], axis=1)
        wide_part = dot(lhs_h[c], both)
        total = wide_part[:, 0:128] + wide_part[:, 128:256] + dot(lhs_l[c], high)
        if c == 0:
            part[it] = total
        else:
            part[it] = part[it] + total

    def far_copy(it, k):
        dz, dy, dg = FAR[k]
        target, core = wide_at(dz, dy), (grp + dg) % 2
        return remote(
            to_far.at[it, target * 2 + core], from_far.at[it, wide * 2 + grp],
            f_send.at[it, k], f_recv.at[it, k], (target, narrow, core),
        )

    def core_copy(it, k):
        dx, dy = (PAIRS + [(0, 0)])[k]
        row = pl.multiple_of(extra + narrow_at(dx, dy) * 128 + (1 - grp) * 64, 32)
        return remote(
            part.at[it, pl.ds(row, 64)], from_core.at[it, k], c_send.at[it, k], c_recv.at[it, k],
            (wide, narrow, 1 - grp),
        )

    def pair_copy(it, k):
        dx, dy = PAIRS[k]
        return remote(
            to_pair.at[it, k], from_pair.at[it, k], p_send.at[it, k], p_recv.at[it, k],
            (wide, narrow_at(dx, dy), grp),
        )

    def sweep(it, first):
        if first:
            chores = [
                functools.partial(split_block, 0), functools.partial(split_block, 1), index_tables,
                functools.partial(split_block, 2), functools.partial(split_block, 3), s_copy.wait,
                functools.partial(split_schur, 0), functools.partial(split_schur, 1),
                functools.partial(split_schur, 2), functools.partial(split_schur, 3),
            ]
        else:
            chores = []
        for step in PLAN:
            if isinstance(step, tuple):
                if chores:
                    chores.pop(0)()
                gather_copy(it, step).wait_recv()
                hand_on(it, step)
            else:
                while chores:
                    chores.pop(0)()
                multiply(it, step)
        for k in range(len(PAIRS) + 1):
            core_copy(it, k).start()
        outgoing = jnp.zeros((128, 256), jnp.float32)
        for core in range(2):
            key = keys[pl.ds(2 * wide + core, 1), :]
            row = lax.broadcasted_iota(jnp.int32, (128, 128), 0)
            pick = jnp.where(row == key, 1.0, 0.0).astype(jnp.bfloat16)[:, 0:share]
            high, low = halves(part[it, core * share : (core + 1) * share])
            outgoing = outgoing + dot(pick, jnp.concatenate([high, low], axis=1))
        outgoing = (outgoing[:, 0:128] + outgoing[:, 128:256]).reshape(32, 4, 128)
        to_far[it] = outgoing
        for k in range(len(FAR)):
            far_copy(it, k).start()
        from_far[it, wide * 2 + grp] = to_far[it, wide * 2 + grp]
        for k in range(len(PAIRS) + 1):
            dx, dy = (PAIRS + [(0, 0)])[k]
            row = pl.multiple_of(extra + narrow_at(dx, dy) * 128 + grp * 64, 32)
            core_copy(it, k).wait_recv()
            value = part[it, pl.ds(row, 64)] + from_core[it, k]
            if k < len(PAIRS):
                to_pair[it, k] = value
                pair_copy(it, k).start()
            else:
                total = value
        for k in range(len(FAR)):
            far_copy(it, k).wait_recv()
        high, low = halves(from_far[it].reshape(128, 128))
        landed = dot(place[...], jnp.concatenate([high, low], axis=1))
        total = total + (landed[:, 0:128] + landed[:, 128:256])
        for k in range(len(PAIRS)):
            pair_copy(it, k).wait_recv()
            total = total + from_pair[it, k]
        residual = exc[0] - total
        out_r[0] = residual
        updated = gath[it, 0] + weight[...] * residual
        out_t[0] = updated
        return updated

    def finish(it):
        for v in SLOTS[1:]:
            gather_copy(it, v).wait_send()
        for k in range(len(PAIRS) + 1):
            core_copy(it, k).wait_send()
        for k in range(len(FAR)):
            far_copy(it, k).wait_send()
        for k in range(len(PAIRS)):
            pair_copy(it, k).wait_send()

    gath[1, 0] = sweep(0, True)
    hand_on(1, (0, 0))

    def later(it, carry):
        updated = sweep(it, False)

        @pl.when(it < ITERS - 1)
        def _():
            gath[it + 1, 0] = updated
            hand_on(it + 1, (0, 0))

        return carry

    lax.fori_loop(1, ITERS, later, 0)
    lax.fori_loop(0, ITERS, lambda it, carry: (finish(it), carry)[1], 0)


def on_device(boundary_block, schur_blocks, interface_rows, live_rows, row_scale, excitation):
    slots, piece, columns = boundary_block.shape
    share, iface = schur_blocks.shape[1:]
    rows = 2 * share + columns
    blocks = iface // share
    q_blocks = jnp.pad(interface_rows.reshape(blocks, share), ((0, 0), (0, 128 - share)))
    f32, dma = jnp.float32, pltpu.SemaphoreType.DMA
    vmem = pl.BlockSpec(memory_space=pltpu.VMEM)
    hbm = pl.BlockSpec(memory_space=pl.ANY)
    pairs = len(PAIRS)
    return pl.pallas_call(
        kernel,
        out_shape=(
            jax.ShapeDtypeStruct(excitation.shape, f32),
            jax.ShapeDtypeStruct(excitation.shape, f32),
        ),
        in_specs=[hbm, hbm, vmem, vmem, pl.BlockSpec(memory_space=pltpu.SMEM), vmem, vmem],
        out_specs=(vmem, vmem),
        scratch_shapes=[
            pltpu.VMEM((slots, piece, columns), f32),
            pltpu.VMEM((2, share, iface), f32),
            pltpu.VMEM((4, rows, 256), jnp.bfloat16),
            pltpu.VMEM((4, rows, 256), jnp.bfloat16),
            pltpu.VMEM((ITERS, slots, piece, 128), f32),
            pltpu.VMEM((ITERS, rows, 128), f32),
            pltpu.VMEM((ITERS, pairs + 1, piece, 128), f32),
            pltpu.VMEM((ITERS, pairs, piece, 128), f32),
            pltpu.VMEM((ITERS, pairs, piece, 128), f32),
            pltpu.VMEM((ITERS, blocks, 4, 128), f32),
            pltpu.VMEM((ITERS, blocks, 4, 128), f32),
            pltpu.VMEM((blocks, 128), jnp.int32),
            pltpu.VMEM((piece, 128), jnp.bfloat16),
            pltpu.VMEM((piece, 128), f32),
            dma((slots + 1,)),
            dma(()),
            dma(()),
            dma((ITERS, slots - 1)),
            dma((ITERS, slots - 1)),
            dma((ITERS, pairs + 1)),
            dma((ITERS, pairs + 1)),
            dma((ITERS, pairs)),
            dma((ITERS, pairs)),
            dma((ITERS, len(FAR))),
            dma((ITERS, len(FAR))),
        ],
        name="sweeps",
        compiler_params=pltpu.CompilerParams(collective_id=0, has_side_effects=True),
    )(boundary_block, schur_blocks, interface_rows, q_blocks, live_rows, row_scale, excitation)


def solution(mesh):
    placed = (
        P(None, ("narrow", "grp"), "wide"),
        P("narrow", ("wide", "grp"), None),
        P("narrow", None),
        P("narrow"),
        P("wide", ("narrow", "grp")),
        P("wide", ("narrow", "grp"), None),
    )
    return jax.shard_map(
        on_device,
        mesh=mesh,
        in_specs=placed,
        out_specs=(P("wide", ("narrow", "grp"), None), P("wide", ("narrow", "grp"), None)),
        check_vma=False,
    )
```

```python
import functools

import jax
import jax.numpy as jnp
from jax import lax
from jax.experimental import pallas as pl
from jax.experimental.pallas import tpu as pltpu
from jax.sharding import PartitionSpec as P

ITERS = 3
RELAX = 0.35
MESH = pl.DeviceIdType.MESH
NZ, NX = 8, 4

SLOTS = [(0, 0), (4, 1), (3, 1), (5, 1), (2, 1), (6, 1), (1, 1), (7, 1)]
SLOTS += [(4, 0), (3, 0), (5, 0), (2, 0), (6, 0), (1, 0), (7, 0), (0, 1)]
SLOT_OF = {v: i for i, v in enumerate(SLOTS)}
PAIRS = [(dx, dy, dg) for dy in (1, 0) for dx in (2, 1, 3, 0) for dg in (1, 0) if (dx, dy, dg) != (0, 0, 0)]
FAR = [
    (dz, dy, dg)
    for dz in (4, 3, 5, 2, 6, 1, 7, 0)
    for dy in (1, 0)
    for dg in (1, 0)
    if (dz, dy, dg) != (0, 0, 0)
]


def halves(value):
    high = value.astype(jnp.bfloat16)
    low = (value - high.astype(jnp.float32)).astype(jnp.bfloat16)
    return high, low


def dot(a, b):
    return jnp.dot(a, b, preferred_element_type=jnp.float32)


def dot_t(a, b):
    return lax.dot_general(a, b, (((1,), (1,)), ((), ())), preferred_element_type=jnp.float32)


def kernel(
    bb, schur, q_row, live, scale, exc, out,
    bload, sboth, lhs, gath, acc, part, from_pair, to_far, from_far,
    q_blocks, keys, place, weight, force, left,
    load_sem, s_send, s_recv, g_send, g_recv, p_send, p_recv, f_send, f_recv,
):
    wide, narrow, grp = lax.axis_index("wide"), lax.axis_index("narrow"), lax.axis_index("grp")
    z, yh, x, yl = wide // 2, wide % 2, narrow // 2, narrow % 2
    share = sboth.shape[1]
    iface = sboth.shape[2]
    extra = 2 * share
    me = wide * 2 + grp
    left_lanes = lax.broadcasted_iota(jnp.int32, (32, 128), 1) < 64

    def wide_at(dz, dy):
        return ((z + dz + NZ) % NZ) * 2 + (yh + dy + 2) % 2

    def narrow_at(dx, dy):
        return ((x + dx) % NX) * 2 + (yl + dy) % 2

    def swap(value):
        return pltpu.roll(value, 64, 1)

    def remote(src, dst, send, recv, device):
        return pltpu.make_async_remote_copy(
            src_ref=src, dst_ref=dst, send_sem=send, recv_sem=recv, device_id=device, device_id_type=MESH
        )

    barrier = pltpu.get_barrier_semaphore()
    for dz, dy, dg in FAR:
        pl.semaphore_signal(
            barrier, inc=1, device_id=(wide_at(dz, dy), narrow, (grp + dg) % 2), device_id_type=MESH
        )
    for dx, dy, dg in PAIRS[:-1]:
        pl.semaphore_signal(
            barrier, inc=1, device_id=(wide, narrow_at(dx, dy), (grp + dg) % 2), device_id_type=MESH
        )

    b_loads = []
    for i, (dz, dy) in enumerate(SLOTS):
        b_loads.append(pltpu.make_async_copy(bb.at[wide_at(-dz, dy)], bload.at[i], load_sem.at[i]))
        b_loads[-1].start()
    s_load = pltpu.make_async_copy(schur.at[0], sboth.at[grp], load_sem.at[len(SLOTS)])
    s_load.start()

    own = jnp.broadcast_to(scale[...], (64, 64))
    diagonal = lax.broadcasted_iota(jnp.int32, (64, 64), 0) == lax.broadcasted_iota(jnp.int32, (64, 64), 1)
    column = RELAX * jnp.sum(jnp.where(diagonal, own, 0.0), axis=1, keepdims=True)
    weight[...] = jnp.where(
        left_lanes, jnp.broadcast_to(column[0:32], (32, 128)), jnp.broadcast_to(column[32:64], (32, 128))
    )
    upper, lower = exc[0, 0:32], exc[0, 32:64]
    force[0] = jnp.where(left_lanes, upper, swap(lower))
    force[1] = jnp.where(left_lanes, swap(upper), lower)
    for h in range(2):
        gath[0, h, 0] = weight[...] * force[h]
    live_count = live[0]

    def gather_copy(it, h, k):
        dz, dy = SLOTS[k]
        return remote(
            gath.at[it, h, 0], gath.at[it, h, k], g_send.at[it, h], g_recv.at[it, h, k - 1],
            (wide_at(dz, dy), narrow, grp),
        )

    def hand_out(it, h):
        for k in range(1, len(SLOTS)):
            gather_copy(it, h, k).start()

    def split_block(c):
        for i in range(4 * c, 4 * c + 4):
            b_loads[i].wait()
        for pair in range(2):
            i = 4 * c + 2 * pair
            block = bload[i : i + 2].reshape(128, bload.shape[2])
            for m in range(0, block.shape[1], 256):
                high, low = halves(block[:, m : m + 256].T)
                lhs[c, pl.ds(extra + m, 256), pl.ds(128 * pair, 128)] = high
                lhs[c, pl.ds(extra + m, 256), pl.ds(256 + 128 * pair, 128)] = low

    def split_schur(c):
        q = q_row[...]
        lane = lax.broadcasted_iota(jnp.int32, (1, iface), 1)
        q = jnp.where(lane < live_count, q, -1)
        rows = []
        for i in range(4 * c, 4 * c + 4):
            dz, dy = SLOTS[i]
            shifted = jnp.broadcast_to(q - (wide_at(-dz, dy) * 128 + grp * 64), (64, iface))
            hit = shifted == lax.broadcasted_iota(jnp.int32, (64, iface), 0)
            rows.append(jnp.where(hit, 1.0, 0.0).astype(jnp.bfloat16))
        picked = jnp.concatenate(rows, axis=0)
        high, low = halves(sboth[...].reshape(extra, iface))
        lhs[c, 0:extra, 0:256] = dot_t(high, picked).astype(jnp.bfloat16)
        lhs[c, 0:extra, 256:512] = dot_t(low, picked).astype(jnp.bfloat16)

    def index_tables():
        blocks = q_blocks.shape[0]
        for b in range(blocks):
            q_blocks[b : b + 1, 0:share] = q_row[:, b * share : (b + 1) * share]
        q = q_blocks[...]
        lane = lax.broadcasted_iota(jnp.int32, (blocks, 128), 1)
        block = lax.broadcasted_iota(jnp.int32, (blocks, 128), 0)
        owner = q // 64
        rank = jnp.zeros_like(q)
        for d in range(1, share):
            same = (pltpu.roll(owner, d, 1) == owner) & (lane >= d)
            rank = rank + jnp.where(same, 1, 0)
        used = (lane < share) & (block * share + lane < live_count)
        keys[...] = jnp.where(used, owner + 32 * rank, -1)
        mine = used & (owner == me)
        row = lax.broadcasted_iota(jnp.int32, (64, 128), 0)
        for level in range(2):
            spot = jnp.where(mine & (rank == level), q % 64 + 1, 0)
            spot = jnp.sum(spot, axis=1, keepdims=True)
            match = (block == 2 * (lane // 4) + lane % 2) & (lane < 64)
            rowpos = jnp.sum(jnp.where(match, spot, 0), axis=0, keepdims=True)
            place[64 * level : 64 * level + 64] = jnp.where(row == rowpos - 1, 1.0, 0.0).astype(jnp.bfloat16)

    def right_side(it, h, c):
        rows = []
        for i in range(4 * c, 4 * c + 4):
            value = gath[it, h, i]
            high = value.astype(jnp.bfloat16).astype(jnp.float32)
            low = value - high
            rows.append(jnp.where(left_lanes, high, swap(low)))
            rows.append(jnp.where(left_lanes, swap(high), low))
        right = jnp.concatenate(rows, axis=0).astype(jnp.bfloat16)
        return jnp.concatenate([right, right], axis=0)

    def multiply(it, h, c):
        total = dot(lhs[c], right_side(it, h, c))
        if c == 0:
            acc[h] = total
        else:
            acc[h] = acc[h] + total

    def far_copy(it, h, k):
        dz, dy, dg = FAR[k]
        target, core = wide_at(dz, dy), (grp + dg) % 2
        return remote(
            to_far.at[it, h, target * 2 + core], from_far.at[it, h, me],
            f_send.at[it, h], f_recv.at[it, h], (target, narrow, core),
        )

    def pair_copy(it, h, k):
        dx, dy, dg = PAIRS[k]
        target, core = narrow_at(dx, dy), (grp + dg) % 2
        return remote(
            part.at[it, h, target * 2 + core], from_pair.at[it, h, k], p_send.at[it, h], p_recv.at[it, h],
            (wide, target, core),
        )

    def send_far(it, h):
        packed = []
        for core in range(2):
            key = keys[pl.ds(2 * wide + core, 1), :]
            row = lax.broadcasted_iota(jnp.int32, (64, 128), 0)
            pick = jnp.where(row == key, 1.0, 0.0).astype(jnp.bfloat16)[:, 0:share]
            value = acc[h, core * share : (core + 1) * share]
            high = value.astype(jnp.bfloat16)
            low = (value - high.astype(jnp.float32)).astype(jnp.bfloat16)
            picked = dot(pick, jnp.concatenate([high, low], axis=1))
            picked = picked[:, 0:128] + picked[:, 128:256]
            picked = picked + swap(picked)
            packed.append(jnp.where(left_lanes, picked[0:32], picked[32:64]))
        to_far[it, h] = jnp.stack(packed, axis=1)
        for k in range(len(FAR)):
            far_copy(it, h, k).start()
        from_far[it, h, me] = to_far[it, h, me]

    def last_multiply(it, h):
        c = len(SLOTS) // 4 - 1
        right = right_side(it, h, c)
        acc[h, 0:extra] = acc[h, 0:extra] + dot(lhs[c, 0:extra], right)
        send_far(it, h)
        total = acc[h, extra:] + dot(lhs[c, extra:], right)
        total = total + swap(total)
        for b in range(16):
            part[it, h, b] = jnp.where(left_lanes, total[64 * b : 64 * b + 32], total[64 * b + 32 : 64 * b + 64])
        for k in range(len(PAIRS)):
            pair_copy(it, h, k).start()

    def update(it, h):
        here = (wide, narrow, grp)
        remote(
            from_pair.at[it, h], from_pair.at[it, h], p_send.at[it, h], p_recv.at[it, h], here
        ).wait_recv()
        total = part[it, h, narrow * 2 + grp]
        for k in range(len(PAIRS)):
            total = total + from_pair[it, h, k]
        far = len(FAR)
        remote(
            to_far.at[it, h, 0:far], from_far.at[it, h, 0:far], f_send.at[it, h], f_recv.at[it, h],
            (wide, narrow, grp),
        ).wait_recv()
        high, low = halves(from_far[it, h].reshape(64, 128))
        landed = dot(place[:, 0:64], jnp.concatenate([high, low], axis=1))
        landed = landed[:, 0:128] + landed[:, 128:256]
        one = jnp.where(left_lanes, landed[0:32], landed[96:128])
        two = jnp.where(left_lanes, landed[32:64], landed[64:96])
        residual = force[h] - (total + one + swap(two))
        updated = gath[it, h, 0] + weight[...] * residual
        return residual, updated

    def strip(it, h):
        for c in range(len(SLOTS) // 4):
            for k in range(max(4 * c, 1), 4 * c + 4):
                gather_copy(it, h, k).wait_recv()
            if 4 * c + 4 < len(SLOTS):
                multiply(it, h, c)
            else:
                last_multiply(it, h)

    def sweep(it, then):
        for h in range(2):
            strip(it, h)
        for h in range(2):
            then(it, h, *update(it, h))

    def go_on(it, h, residual, updated):
        gath[it + 1, h, 0] = updated
        hand_out(it + 1, h)

    def keep(it, h, residual, updated):
        force[h] = residual
        left[h] = updated

    def finish(it, carry):
        for h in range(2):
            here = (wide, narrow, grp)
            remote(
                gath.at[it, h, 1:], gath.at[it, h, 1:], g_send.at[it, h], g_recv.at[it, h, 0], here
            ).wait_send()
            remote(
                from_pair.at[it, h], from_pair.at[it, h], p_send.at[it, h], p_recv.at[it, h], here
            ).wait_send()
            far = len(FAR)
            remote(
                to_far.at[it, h, 0:far], from_far.at[it, h, 0:far], f_send.at[it, h], f_recv.at[it, h], here
            ).wait_send()
        return carry

    index_tables()
    split_block(0)
    split_block(1)
    pl.semaphore_wait(barrier, len(FAR) + len(PAIRS) - 1)
    hand_out(0, 0)
    hand_out(0, 1)
    s_load.wait()
    s_copy = remote(sboth.at[grp], sboth.at[grp], s_send, s_recv, (wide, narrow, 1 - grp))
    s_copy.start()
    chores = [functools.partial(split_block, 2), functools.partial(split_block, 3), s_copy.wait]
    chores += [functools.partial(split_schur, c) for c in range(4)]
    for chore in chores:
        chore()
    sweep(0, go_on)

    def middle(it, carry):
        sweep(it, go_on)
        return carry

    lax.fori_loop(1, ITERS - 1, middle, 0)
    sweep(ITERS - 1, keep)
    for i, value in enumerate((left, force)):
        out[i, 0:32] = jnp.where(left_lanes, value[0], swap(value[1]))
        out[i, 32:64] = jnp.where(left_lanes, swap(value[0]), value[1])
    lax.fori_loop(0, ITERS, finish, 0)


def on_device(boundary_block, schur_blocks, interface_rows, live_rows, row_scale, excitation):
    slots, piece, columns = boundary_block.shape
    share, iface = schur_blocks.shape[1:]
    rows = 2 * share + columns
    blocks = iface // share
    f32, dma = jnp.float32, pltpu.SemaphoreType.DMA
    vmem = pl.BlockSpec(memory_space=pltpu.VMEM)
    hbm = pl.BlockSpec(memory_space=pl.ANY)
    pairs = len(PAIRS)
    both = pl.pallas_call(
        kernel,
        out_shape=jax.ShapeDtypeStruct((2, piece, 128), f32),
        in_specs=[hbm, hbm, vmem, pl.BlockSpec(memory_space=pltpu.SMEM), vmem, vmem],
        out_specs=vmem,
        scratch_shapes=[
            pltpu.VMEM((slots, piece, columns), f32),
            pltpu.VMEM((2, share, iface), f32),
            pltpu.VMEM((slots // 4, rows, 512), jnp.bfloat16),
            pltpu.VMEM((ITERS, 2, slots, piece // 2, 128), f32),
            pltpu.VMEM((2, rows, 128), f32),
            pltpu.VMEM((ITERS, 2, slots, piece // 2, 128), f32),
            pltpu.VMEM((ITERS, 2, pairs, piece // 2, 128), f32),
            pltpu.VMEM((ITERS, 2, blocks, 2, 128), f32),
            pltpu.VMEM((ITERS, 2, blocks, 2, 128), f32),
            pltpu.VMEM((blocks, 128), jnp.int32),
            pltpu.VMEM((blocks, 128), jnp.int32),
            pltpu.VMEM((2 * piece, 128), jnp.bfloat16),
            pltpu.VMEM((piece // 2, 128), f32),
            pltpu.VMEM((2, piece // 2, 128), f32),
            pltpu.VMEM((2, piece // 2, 128), f32),
            dma((slots + 1,)),
            dma(()),
            dma(()),
            dma((ITERS, 2)),
            dma((ITERS, 2, slots - 1)),
            dma((ITERS, 2)),
            dma((ITERS, 2)),
            dma((ITERS, 2)),
            dma((ITERS, 2)),
        ],
        name="sweeps",
        compiler_params=pltpu.CompilerParams(collective_id=0, has_side_effects=True),
    )(boundary_block, schur_blocks, interface_rows, live_rows, row_scale, excitation)
    return both[0:1], both[1:2]


def solution(mesh):
    placed = (
        P(None, ("narrow", "grp"), "wide"),
        P("narrow", ("wide", "grp"), None),
        P("narrow", None),
        P("narrow"),
        P("wide", ("narrow", "grp")),
        P("wide", ("narrow", "grp"), None),
    )
    return jax.shard_map(
        on_device,
        mesh=mesh,
        in_specs=placed,
        out_specs=(P("wide", ("narrow", "grp"), None), P("wide", ("narrow", "grp"), None)),
        check_vma=False,
    )
```

```python
import functools

import jax
import jax.numpy as jnp
from jax import lax
from jax.experimental import pallas as pl
from jax.experimental.pallas import tpu as pltpu
from jax.sharding import PartitionSpec as P

ITERS = 3
RELAX = 0.35
MESH = pl.DeviceIdType.MESH
NZ, NX = 8, 4

SLOTS = [(0, 0), (4, 1), (3, 1), (5, 1), (2, 1), (6, 1), (1, 1), (7, 1)]
SLOTS += [(4, 0), (3, 0), (5, 0), (2, 0), (6, 0), (1, 0), (7, 0), (0, 1)]
SLOT_OF = {v: i for i, v in enumerate(SLOTS)}
PAIRS = [(dx, dy, dg) for dy in (1, 0) for dx in (2, 1, 3, 0) for dg in (1, 0) if (dx, dy, dg) != (0, 0, 0)]
FAR = [
    (dz, dy, dg)
    for dz in (4, 3, 5, 2, 6, 1, 7, 0)
    for dy in (1, 0)
    for dg in (1, 0)
    if (dz, dy, dg) != (0, 0, 0)
]


def halves(value):
    high = value.astype(jnp.bfloat16)
    low = (value - high.astype(jnp.float32)).astype(jnp.bfloat16)
    return high, low


def dot(a, b):
    return jnp.dot(a, b, preferred_element_type=jnp.float32)


def dot_t(a, b):
    return lax.dot_general(a, b, (((1,), (1,)), ((), ())), preferred_element_type=jnp.float32)


def kernel(
    bb, schur, q_hbm, live, scale_hbm, exc_hbm, out,
    bload, sboth, lhs, gath, acc, part, from_pair, to_far, from_far,
    q_row, scale, exc, q_blocks, keys, place, weight, force, left,
    load_sem, s_send, s_recv, g_send, g_recv, p_send, p_recv, f_send, f_recv,
):
    wide, narrow, grp = lax.axis_index("wide"), lax.axis_index("narrow"), lax.axis_index("grp")
    z, yh, x, yl = wide // 2, wide % 2, narrow // 2, narrow % 2
    share = sboth.shape[1]
    iface = sboth.shape[2]
    extra = 2 * share
    me = wide * 2 + grp
    left_lanes = lax.broadcasted_iota(jnp.int32, (32, 128), 1) < 64

    def wide_at(dz, dy):
        return ((z + dz + NZ) % NZ) * 2 + (yh + dy + 2) % 2

    def narrow_at(dx, dy):
        return ((x + dx) % NX) * 2 + (yl + dy) % 2

    def swap(value):
        return pltpu.roll(value, 64, 1)

    def remote(src, dst, send, recv, device):
        return pltpu.make_async_remote_copy(
            src_ref=src, dst_ref=dst, send_sem=send, recv_sem=recv, device_id=device, device_id_type=MESH
        )

    small = [
        pltpu.make_async_copy(src, dst, load_sem.at[len(SLOTS) + 1 + i])
        for i, (src, dst) in enumerate(((exc_hbm, exc), (scale_hbm, scale), (q_hbm, q_row)))
    ]
    for copy in small:
        copy.start()
    barrier = pltpu.get_barrier_semaphore()
    for dz, dy, dg in FAR:
        pl.semaphore_signal(
            barrier, inc=1, device_id=(wide_at(dz, dy), narrow, (grp + dg) % 2), device_id_type=MESH
        )
    for dx, dy, dg in PAIRS[:-1]:
        pl.semaphore_signal(
            barrier, inc=1, device_id=(wide, narrow_at(dx, dy), (grp + dg) % 2), device_id_type=MESH
        )

    b_loads = []
    for i, (dz, dy) in enumerate(SLOTS):
        b_loads.append(pltpu.make_async_copy(bb.at[wide_at(-dz, dy)], bload.at[i], load_sem.at[i]))
        b_loads[-1].start()
    s_load = pltpu.make_async_copy(schur.at[0], sboth.at[grp], load_sem.at[len(SLOTS)])
    s_load.start()

    for copy in small:
        copy.wait()
    own = jnp.broadcast_to(scale[...], (64, 64))
    diagonal = lax.broadcasted_iota(jnp.int32, (64, 64), 0) == lax.broadcasted_iota(jnp.int32, (64, 64), 1)
    column = RELAX * jnp.sum(jnp.where(diagonal, own, 0.0), axis=1, keepdims=True)
    weight[...] = jnp.where(
        left_lanes, jnp.broadcast_to(column[0:32], (32, 128)), jnp.broadcast_to(column[32:64], (32, 128))
    )
    upper, lower = exc[0, 0:32], exc[0, 32:64]
    force[0] = jnp.where(left_lanes, upper, swap(lower))
    force[1] = jnp.where(left_lanes, swap(upper), lower)
    for h in range(2):
        gath[0, h, 0] = weight[...] * force[h]
    live_count = live[0]

    def gather_copy(it, h, k):
        dz, dy = SLOTS[k]
        return remote(
            gath.at[it, h, 0], gath.at[it, h, k], g_send.at[it, h], g_recv.at[it, h, k - 1],
            (wide_at(dz, dy), narrow, grp),
        )

    def hand_out(it, h):
        for k in range(1, len(SLOTS)):
            gather_copy(it, h, k).start()

    def split_block(c):
        for i in range(4 * c, 4 * c + 4):
            b_loads[i].wait()
        for pair in range(2):
            i = 4 * c + 2 * pair
            block = bload[i : i + 2].reshape(128, bload.shape[2])
            for m in range(0, block.shape[1], 256):
                high, low = halves(block[:, m : m + 256].T)
                lhs[c, pl.ds(extra + m, 256), pl.ds(128 * pair, 128)] = high
                lhs[c, pl.ds(extra + m, 256), pl.ds(256 + 128 * pair, 128)] = low

    def split_schur(c):
        q = q_row[...]
        lane = lax.broadcasted_iota(jnp.int32, (1, iface), 1)
        q = jnp.where(lane < live_count, q, -1)
        rows = []
        for i in range(4 * c, 4 * c + 4):
            dz, dy = SLOTS[i]
            shifted = jnp.broadcast_to(q - (wide_at(-dz, dy) * 128 + grp * 64), (64, iface))
            hit = shifted == lax.broadcasted_iota(jnp.int32, (64, iface), 0)
            rows.append(jnp.where(hit, 1.0, 0.0).astype(jnp.bfloat16))
        picked = jnp.concatenate(rows, axis=0)
        high, low = halves(sboth[...].reshape(extra, iface))
        lhs[c, 0:extra, 0:256] = dot_t(high, picked).astype(jnp.bfloat16)
        lhs[c, 0:extra, 256:512] = dot_t(low, picked).astype(jnp.bfloat16)

    def index_tables():
        blocks = q_blocks.shape[0]
        for b in range(blocks):
            q_blocks[b : b + 1, 0:share] = q_row[:, b * share : (b + 1) * share]
        q = q_blocks[...]
        lane = lax.broadcasted_iota(jnp.int32, (blocks, 128), 1)
        block = lax.broadcasted_iota(jnp.int32, (blocks, 128), 0)
        owner = q // 64
        rank = jnp.zeros_like(q)
        for d in range(1, share):
            same = (pltpu.roll(owner, d, 1) == owner) & (lane >= d)
            rank = rank + jnp.where(same, 1, 0)
        used = (lane < share) & (block * share + lane < live_count)
        keys[...] = jnp.where(used, owner + 32 * rank, -1)
        mine = used & (owner == me)
        row = lax.broadcasted_iota(jnp.int32, (64, 128), 0)
        for level in range(2):
            spot = jnp.where(mine & (rank == level), q % 64 + 1, 0)
            spot = jnp.sum(spot, axis=1, keepdims=True)
            match = (block == 2 * (lane // 4) + lane % 2) & (lane < 64)
            rowpos = jnp.sum(jnp.where(match, spot, 0), axis=0, keepdims=True)
            place[64 * level : 64 * level + 64] = jnp.where(row == rowpos - 1, 1.0, 0.0).astype(jnp.bfloat16)

    def right_side(it, h, c):
        rows = []
        for i in range(4 * c, 4 * c + 4):
            value = gath[it, h, i]
            high = value.astype(jnp.bfloat16).astype(jnp.float32)
            low = value - high
            rows.append(jnp.where(left_lanes, high, swap(low)))
            rows.append(jnp.where(left_lanes, swap(high), low))
        right = jnp.concatenate(rows, axis=0).astype(jnp.bfloat16)
        return jnp.concatenate([right, right], axis=0)

    def multiply(it, h, c):
        total = dot(lhs[c], right_side(it, h, c))
        if c == 0:
            acc[h] = total
        else:
            acc[h] = acc[h] + total

    def far_copy(it, h, k):
        dz, dy, dg = FAR[k]
        target, core = wide_at(dz, dy), (grp + dg) % 2
        return remote(
            to_far.at[it, h, target * 2 + core], from_far.at[it, h, me],
            f_send.at[it, h], f_recv.at[it, h], (target, narrow, core),
        )

    def pair_copy(it, h, k):
        dx, dy, dg = PAIRS[k]
        target, core = narrow_at(dx, dy), (grp + dg) % 2
        return remote(
            part.at[it, h, target * 2 + core], from_pair.at[it, h, k], p_send.at[it, h], p_recv.at[it, h],
            (wide, target, core),
        )

    def send_far(it, h):
        packed = []
        for core in range(2):
            key = keys[pl.ds(2 * wide + core, 1), :]
            row = lax.broadcasted_iota(jnp.int32, (64, 128), 0)
            pick = jnp.where(row == key, 1.0, 0.0).astype(jnp.bfloat16)[:, 0:share]
            value = acc[h, core * share : (core + 1) * share]
            high = value.astype(jnp.bfloat16)
            low = (value - high.astype(jnp.float32)).astype(jnp.bfloat16)
            picked = dot(pick, jnp.concatenate([high, low], axis=1))
            picked = picked[:, 0:128] + picked[:, 128:256]
            picked = picked + swap(picked)
            packed.append(jnp.where(left_lanes, picked[0:32], picked[32:64]))
        to_far[it, h] = jnp.stack(packed, axis=1)
        for k in range(len(FAR)):
            far_copy(it, h, k).start()
        from_far[it, h, me] = to_far[it, h, me]

    def last_multiply(it, h):
        c = len(SLOTS) // 4 - 1
        right = right_side(it, h, c)
        acc[h, 0:extra] = acc[h, 0:extra] + dot(lhs[c, 0:extra], right)
        send_far(it, h)
        for dx in (2, 1, 3, 0):
            target = (x + dx) % NX
            row = pl.multiple_of(extra + target * 256, 32)
            total = acc[h, pl.ds(row, 256)] + dot(lhs[c, pl.ds(row, 256)], right)
            total = total + swap(total)
            for b in range(4):
                upper, lower = total[64 * b : 64 * b + 32], total[64 * b + 32 : 64 * b + 64]
                part[it, h, target * 4 + b] = jnp.where(left_lanes, upper, lower)
            for k in range(len(PAIRS)):
                if PAIRS[k][0] == dx:
                    pair_copy(it, h, k).start()

    def update(it, h):
        here = (wide, narrow, grp)
        far = len(FAR)
        remote(
            to_far.at[it, h, 0:far], from_far.at[it, h, 0:far], f_send.at[it, h], f_recv.at[it, h],
            (wide, narrow, grp),
        ).wait_recv()
        high, low = halves(from_far[it, h].reshape(64, 128))
        landed = dot(place[:, 0:64], jnp.concatenate([high, low], axis=1))
        landed = landed[:, 0:128] + landed[:, 128:256]
        remote(
            from_pair.at[it, h], from_pair.at[it, h], p_send.at[it, h], p_recv.at[it, h], here
        ).wait_recv()
        total = part[it, h, narrow * 2 + grp]
        for k in range(len(PAIRS)):
            total = total + from_pair[it, h, k]
        one = jnp.where(left_lanes, landed[0:32], landed[96:128])
        two = jnp.where(left_lanes, landed[32:64], landed[64:96])
        residual = force[h] - (total + one + swap(two))
        updated = gath[it, h, 0] + weight[...] * residual
        return residual, updated

    def strip(it, h):
        for c in range(len(SLOTS) // 4):
            for k in range(max(4 * c, 1), 4 * c + 4):
                gather_copy(it, h, k).wait_recv()
            if 4 * c + 4 < len(SLOTS):
                multiply(it, h, c)
            else:
                last_multiply(it, h)

    def sweep(it, then):
        for h in range(2):
            strip(it, h)
        for h in range(2):
            then(it, h, *update(it, h))

    def go_on(it, h, residual, updated):
        gath[it + 1, h, 0] = updated
        hand_out(it + 1, h)

    def keep(it, h, residual, updated):
        force[h] = residual
        left[h] = updated

    def finish(it, carry):
        for h in range(2):
            here = (wide, narrow, grp)
            remote(
                gath.at[it, h, 1:], gath.at[it, h, 1:], g_send.at[it, h], g_recv.at[it, h, 0], here
            ).wait_send()
            remote(
                from_pair.at[it, h], from_pair.at[it, h], p_send.at[it, h], p_recv.at[it, h], here
            ).wait_send()
            far = len(FAR)
            remote(
                to_far.at[it, h, 0:far], from_far.at[it, h, 0:far], f_send.at[it, h], f_recv.at[it, h], here
            ).wait_send()
        return carry

    index_tables()
    split_block(0)
    split_block(1)
    pl.semaphore_wait(barrier, len(FAR) + len(PAIRS) - 1)
    hand_out(0, 0)
    hand_out(0, 1)
    s_load.wait()
    s_copy = remote(sboth.at[grp], sboth.at[grp], s_send, s_recv, (wide, narrow, 1 - grp))
    s_copy.start()
    chores = [functools.partial(split_block, 2), functools.partial(split_block, 3), s_copy.wait]
    chores += [functools.partial(split_schur, c) for c in range(4)]
    for chore in chores:
        chore()
    sweep(0, go_on)

    def middle(it, carry):
        sweep(it, go_on)
        return carry

    lax.fori_loop(1, ITERS - 1, middle, 0)
    sweep(ITERS - 1, keep)
    for i, value in enumerate((left, force)):
        out[i, 0:32] = jnp.where(left_lanes, value[0], swap(value[1]))
        out[i, 32:64] = jnp.where(left_lanes, swap(value[0]), value[1])
    lax.fori_loop(0, ITERS, finish, 0)


def on_device(boundary_block, schur_blocks, interface_rows, live_rows, row_scale, excitation):
    slots, piece, columns = boundary_block.shape
    share, iface = schur_blocks.shape[1:]
    rows = 2 * share + columns
    blocks = iface // share
    f32, dma = jnp.float32, pltpu.SemaphoreType.DMA
    vmem = pl.BlockSpec(memory_space=pltpu.VMEM)
    hbm = pl.BlockSpec(memory_space=pl.ANY)
    pairs = len(PAIRS)
    both = pl.pallas_call(
        kernel,
        out_shape=jax.ShapeDtypeStruct((2, piece, 128), f32),
        in_specs=[hbm, hbm, hbm, pl.BlockSpec(memory_space=pltpu.SMEM), hbm, hbm],
        out_specs=vmem,
        scratch_shapes=[
            pltpu.VMEM((slots, piece, columns), f32),
            pltpu.VMEM((2, share, iface), f32),
            pltpu.VMEM((slots // 4, rows, 512), jnp.bfloat16),
            pltpu.VMEM((ITERS, 2, slots, piece // 2, 128), f32),
            pltpu.VMEM((2, rows, 128), f32),
            pltpu.VMEM((ITERS, 2, slots, piece // 2, 128), f32),
            pltpu.VMEM((ITERS, 2, pairs, piece // 2, 128), f32),
            pltpu.VMEM((ITERS, 2, blocks, 2, 128), f32),
            pltpu.VMEM((ITERS, 2, blocks, 2, 128), f32),
            pltpu.VMEM((1, iface), jnp.int32),
            pltpu.VMEM((1, piece), f32),
            pltpu.VMEM((1, piece, 128), f32),
            pltpu.VMEM((blocks, 128), jnp.int32),
            pltpu.VMEM((blocks, 128), jnp.int32),
            pltpu.VMEM((2 * piece, 128), jnp.bfloat16),
            pltpu.VMEM((piece // 2, 128), f32),
            pltpu.VMEM((2, piece // 2, 128), f32),
            pltpu.VMEM((2, piece // 2, 128), f32),
            dma((slots + 4,)),
            dma(()),
            dma(()),
            dma((ITERS, 2)),
            dma((ITERS, 2, slots - 1)),
            dma((ITERS, 2)),
            dma((ITERS, 2)),
            dma((ITERS, 2)),
            dma((ITERS, 2)),
        ],
        name="sweeps",
        compiler_params=pltpu.CompilerParams(collective_id=0, has_side_effects=True),
    )(boundary_block, schur_blocks, interface_rows, live_rows, row_scale, excitation)
    return both[0:1], both[1:2]


def solution(mesh):
    placed = (
        P(None, ("narrow", "grp"), "wide"),
        P("narrow", ("wide", "grp"), None),
        P("narrow", None),
        P("narrow"),
        P("wide", ("narrow", "grp")),
        P("wide", ("narrow", "grp"), None),
    )
    return jax.shard_map(
        on_device,
        mesh=mesh,
        in_specs=placed,
        out_specs=(P("wide", ("narrow", "grp"), None), P("wide", ("narrow", "grp"), None)),
        check_vma=False,
    )
```

```python
import functools

import jax
import jax.numpy as jnp
from jax import lax
from jax.experimental import pallas as pl
from jax.experimental.pallas import tpu as pltpu
from jax.sharding import PartitionSpec as P

ITERS = 3
RELAX = 0.35
MESH = pl.DeviceIdType.MESH
NZ, NX = 8, 4

SLOTS = [(0, 0), (4, 1), (3, 1), (5, 1), (2, 1), (6, 1), (1, 1), (7, 1)]
SLOTS += [(4, 0), (3, 0), (5, 0), (2, 0), (6, 0), (1, 0), (7, 0), (0, 1)]
SLOT_OF = {v: i for i, v in enumerate(SLOTS)}
PAIRS = [(dx, dy, dg) for dy in (1, 0) for dx in (2, 1, 3, 0) for dg in (1, 0) if (dx, dy, dg) != (0, 0, 0)]
FAR = [
    (dz, dy, dg)
    for dz in (4, 3, 5, 2, 6, 1, 7, 0)
    for dy in (1, 0)
    for dg in (1, 0)
    if (dz, dy, dg) != (0, 0, 0)
]


def halves(value):
    high = value.astype(jnp.bfloat16)
    low = (value - high.astype(jnp.float32)).astype(jnp.bfloat16)
    return high, low


def dot(a, b):
    return jnp.dot(a, b, preferred_element_type=jnp.float32)


def dot_t(a, b):
    return lax.dot_general(a, b, (((1,), (1,)), ((), ())), preferred_element_type=jnp.float32)


def kernel(
    bb, schur, q_hbm, live, scale_hbm, exc_hbm, out,
    bload, sboth, lhs, gath, acc, part, from_pair, to_far, from_far,
    q_row, scale, exc, q_blocks, keys, place, weight, force, left,
    load_sem, s_send, s_recv, g_send, g_recv, p_send, p_recv, f_send, f_recv,
):
    wide, narrow, grp = lax.axis_index("wide"), lax.axis_index("narrow"), lax.axis_index("grp")
    z, yh, x, yl = wide // 2, wide % 2, narrow // 2, narrow % 2
    share = sboth.shape[1]
    iface = sboth.shape[2]
    extra = 2 * share
    me = wide * 2 + grp
    left_lanes = lax.broadcasted_iota(jnp.int32, (32, 128), 1) < 64

    def wide_at(dz, dy):
        return ((z + dz + NZ) % NZ) * 2 + (yh + dy + 2) % 2

    def narrow_at(dx, dy):
        return ((x + dx) % NX) * 2 + (yl + dy) % 2

    def swap(value):
        return pltpu.roll(value, 64, 1)

    def remote(src, dst, send, recv, device):
        return pltpu.make_async_remote_copy(
            src_ref=src, dst_ref=dst, send_sem=send, recv_sem=recv, device_id=device, device_id_type=MESH
        )

    small = [
        pltpu.make_async_copy(src, dst, load_sem.at[len(SLOTS) + 1 + i])
        for i, (src, dst) in enumerate(((exc_hbm, exc), (scale_hbm, scale), (q_hbm, q_row)))
    ]
    for copy in small:
        copy.start()
    barrier = pltpu.get_barrier_semaphore()
    for dz, dy, dg in FAR:
        pl.semaphore_signal(
            barrier, inc=1, device_id=(wide_at(dz, dy), narrow, (grp + dg) % 2), device_id_type=MESH
        )
    for dx, dy, dg in PAIRS[:-1]:
        pl.semaphore_signal(
            barrier, inc=1, device_id=(wide, narrow_at(dx, dy), (grp + dg) % 2), device_id_type=MESH
        )

    b_loads = []
    for i, (dz, dy) in enumerate(SLOTS):
        b_loads.append(pltpu.make_async_copy(bb.at[wide_at(-dz, dy)], bload.at[i], load_sem.at[i]))
        b_loads[-1].start()
    s_load = pltpu.make_async_copy(schur.at[0], sboth.at[grp], load_sem.at[len(SLOTS)])
    s_load.start()

    for copy in small:
        copy.wait()
    own = jnp.broadcast_to(scale[...], (64, 64))
    diagonal = lax.broadcasted_iota(jnp.int32, (64, 64), 0) == lax.broadcasted_iota(jnp.int32, (64, 64), 1)
    column = RELAX * jnp.sum(jnp.where(diagonal, own, 0.0), axis=1, keepdims=True)
    weight[...] = jnp.where(
        left_lanes, jnp.broadcast_to(column[0:32], (32, 128)), jnp.broadcast_to(column[32:64], (32, 128))
    )
    upper, lower = exc[0, 0:32], exc[0, 32:64]
    force[0] = jnp.where(left_lanes, upper, swap(lower))
    force[1] = jnp.where(left_lanes, swap(upper), lower)
    for h in range(2):
        gath[0, h, 0] = weight[...] * force[h]
    live_count = live[0]

    def gather_copy(it, h, k):
        dz, dy = SLOTS[k]
        return remote(
            gath.at[it, h, 0], gath.at[it, h, k], g_send.at[it, h], g_recv.at[it, h, k - 1],
            (wide_at(dz, dy), narrow, grp),
        )

    def hand_out(it, h):
        for k in range(1, len(SLOTS)):
            gather_copy(it, h, k).start()

    def split_block(c):
        for i in range(4 * c, 4 * c + 4):
            b_loads[i].wait()
        for pair in range(2):
            i = 4 * c + 2 * pair
            block = bload[i : i + 2].reshape(128, bload.shape[2])
            for m in range(0, block.shape[1], 256):
                high, low = halves(block[:, m : m + 256].T)
                lhs[c, pl.ds(extra + m, 256), pl.ds(128 * pair, 128)] = high
                lhs[c, pl.ds(extra + m, 256), pl.ds(256 + 128 * pair, 128)] = low

    def split_schur(c):
        q = q_row[...]
        lane = lax.broadcasted_iota(jnp.int32, (1, iface), 1)
        q = jnp.where(lane < live_count, q, -1)
        rows = []
        for i in range(4 * c, 4 * c + 4):
            dz, dy = SLOTS[i]
            shifted = jnp.broadcast_to(q - (wide_at(-dz, dy) * 128 + grp * 64), (64, iface))
            hit = shifted == lax.broadcasted_iota(jnp.int32, (64, iface), 0)
            rows.append(jnp.where(hit, 1.0, 0.0).astype(jnp.bfloat16))
        picked = jnp.concatenate(rows, axis=0)
        high, low = halves(sboth[...].reshape(extra, iface))
        lhs[c, 0:extra, 0:256] = dot_t(high, picked).astype(jnp.bfloat16)
        lhs[c, 0:extra, 256:512] = dot_t(low, picked).astype(jnp.bfloat16)

    def index_tables():
        blocks = q_blocks.shape[0]
        for b in range(blocks):
            q_blocks[b : b + 1, 0:share] = q_row[:, b * share : (b + 1) * share]
        q = q_blocks[...]
        lane = lax.broadcasted_iota(jnp.int32, (blocks, 128), 1)
        block = lax.broadcasted_iota(jnp.int32, (blocks, 128), 0)
        owner = q // 64
        rank = jnp.zeros_like(q)
        for d in range(1, share):
            same = (pltpu.roll(owner, d, 1) == owner) & (lane >= d)
            rank = rank + jnp.where(same, 1, 0)
        used = (lane < share) & (block * share + lane < live_count)
        keys[...] = jnp.where(used, owner + 32 * rank, -1)
        mine = used & (owner == me)
        row = lax.broadcasted_iota(jnp.int32, (64, 128), 0)
        for level in range(2):
            spot = jnp.where(mine & (rank == level), q % 64 + 1, 0)
            spot = jnp.sum(spot, axis=1, keepdims=True)
            match = (block == 2 * (lane // 4) + lane % 2) & (lane < 64)
            rowpos = jnp.sum(jnp.where(match, spot, 0), axis=0, keepdims=True)
            place[64 * level : 64 * level + 64] = jnp.where(row == rowpos - 1, 1.0, 0.0).astype(jnp.bfloat16)

    def right_side(it, h, c):
        rows = []
        for i in range(4 * c, 4 * c + 4):
            value = gath[it, h, i]
            high = value.astype(jnp.bfloat16).astype(jnp.float32)
            low = value - high
            rows.append(jnp.where(left_lanes, high, swap(low)))
            rows.append(jnp.where(left_lanes, swap(high), low))
        right = jnp.concatenate(rows, axis=0).astype(jnp.bfloat16)
        return jnp.concatenate([right, right], axis=0)

    def multiply(it, h, c):
        total = dot(lhs[c], right_side(it, h, c))
        if c == 0:
            acc[h] = total
        else:
            acc[h] = acc[h] + total

    def far_copy(it, h, k):
        dz, dy, dg = FAR[k]
        target, core = wide_at(dz, dy), (grp + dg) % 2
        return remote(
            to_far.at[it, h, target * 2 + core], from_far.at[it, h, me],
            f_send.at[it, h], f_recv.at[it, h], (target, narrow, core),
        )

    def pair_copy(it, h, k):
        dx, dy, dg = PAIRS[k]
        target, core = narrow_at(dx, dy), (grp + dg) % 2
        return remote(
            part.at[it, h, target * 2 + core], from_pair.at[it, h, k], p_send.at[it, h], p_recv.at[it, h],
            (wide, target, core),
        )

    def send_far(it, h):
        packed = []
        for core in range(2):
            key = keys[pl.ds(2 * wide + core, 1), :]
            row = lax.broadcasted_iota(jnp.int32, (64, 128), 0)
            pick = jnp.where(row == key, 1.0, 0.0).astype(jnp.bfloat16)[:, 0:share]
            value = acc[h, core * share : (core + 1) * share]
            high = value.astype(jnp.bfloat16)
            low = (value - high.astype(jnp.float32)).astype(jnp.bfloat16)
            picked = dot(pick, jnp.concatenate([high, low], axis=1))
            picked = picked[:, 0:128] + picked[:, 128:256]
            picked = picked + swap(picked)
            packed.append(jnp.where(left_lanes, picked[0:32], picked[32:64]))
        to_far[it, h] = jnp.stack(packed, axis=1)
        for k in range(len(FAR)):
            far_copy(it, h, k).start()
        from_far[it, h, me] = to_far[it, h, me]

    def last_multiply(it, h):
        c = len(SLOTS) // 4 - 1
        right = right_side(it, h, c)
        acc[h, 0:extra] = acc[h, 0:extra] + dot(lhs[c, 0:extra], right)
        for dx in (2, 1, 3, 0):
            target = (x + dx) % NX
            row = pl.multiple_of(extra + target * 256, 32)
            total = acc[h, pl.ds(row, 256)] + dot(lhs[c, pl.ds(row, 256)], right)
            total = total + swap(total)
            for b in range(4):
                upper, lower = total[64 * b : 64 * b + 32], total[64 * b + 32 : 64 * b + 64]
                part[it, h, target * 4 + b] = jnp.where(left_lanes, upper, lower)
            for k in range(len(PAIRS)):
                if PAIRS[k][0] == dx:
                    pair_copy(it, h, k).start()
            if dx == 2:
                send_far(it, h)

    def update(it, h):
        here = (wide, narrow, grp)
        far = len(FAR)
        remote(
            to_far.at[it, h, 0:far], from_far.at[it, h, 0:far], f_send.at[it, h], f_recv.at[it, h],
            (wide, narrow, grp),
        ).wait_recv()
        high, low = halves(from_far[it, h].reshape(64, 128))
        landed = dot(place[:, 0:64], jnp.concatenate([high, low], axis=1))
        landed = landed[:, 0:128] + landed[:, 128:256]
        remote(
            from_pair.at[it, h], from_pair.at[it, h], p_send.at[it, h], p_recv.at[it, h], here
        ).wait_recv()
        total = part[it, h, narrow * 2 + grp]
        for k in range(len(PAIRS)):
            total = total + from_pair[it, h, k]
        one = jnp.where(left_lanes, landed[0:32], landed[96:128])
        two = jnp.where(left_lanes, landed[32:64], landed[64:96])
        residual = force[h] - (total + one + swap(two))
        updated = gath[it, h, 0] + weight[...] * residual
        return residual, updated

    def strip(it, h):
        for c in range(len(SLOTS) // 4):
            for k in range(max(4 * c, 1), 4 * c + 4):
                gather_copy(it, h, k).wait_recv()
            if 4 * c + 4 < len(SLOTS):
                multiply(it, h, c)
            else:
                last_multiply(it, h)

    def sweep(it, then):
        for h in range(2):
            strip(it, h)
        for h in range(2):
            then(it, h, *update(it, h))

    def go_on(it, h, residual, updated):
        gath[it + 1, h, 0] = updated
        hand_out(it + 1, h)

    def keep(it, h, residual, updated):
        force[h] = residual
        left[h] = updated

    def finish(it, carry):
        for h in range(2):
            here = (wide, narrow, grp)
            remote(
                gath.at[it, h, 1:], gath.at[it, h, 1:], g_send.at[it, h], g_recv.at[it, h, 0], here
            ).wait_send()
            remote(
                from_pair.at[it, h], from_pair.at[it, h], p_send.at[it, h], p_recv.at[it, h], here
            ).wait_send()
            far = len(FAR)
            remote(
                to_far.at[it, h, 0:far], from_far.at[it, h, 0:far], f_send.at[it, h], f_recv.at[it, h], here
            ).wait_send()
        return carry

    index_tables()
    split_block(0)
    split_block(1)
    split_block(2)
    split_block(3)
    pl.semaphore_wait(barrier, len(FAR) + len(PAIRS) - 1)
    hand_out(0, 0)
    hand_out(0, 1)
    s_load.wait()
    s_copy = remote(sboth.at[grp], sboth.at[grp], s_send, s_recv, (wide, narrow, 1 - grp))
    s_copy.start()
    chores = [s_copy.wait]
    chores += [functools.partial(split_schur, c) for c in range(4)]
    for chore in chores:
        chore()
    sweep(0, go_on)

    def middle(it, carry):
        sweep(it, go_on)
        return carry

    lax.fori_loop(1, ITERS - 1, middle, 0)
    sweep(ITERS - 1, keep)
    for i, value in enumerate((left, force)):
        out[i, 0:32] = jnp.where(left_lanes, value[0], swap(value[1]))
        out[i, 32:64] = jnp.where(left_lanes, swap(value[0]), value[1])
    lax.fori_loop(0, ITERS, finish, 0)


def on_device(boundary_block, schur_blocks, interface_rows, live_rows, row_scale, excitation):
    slots, piece, columns = boundary_block.shape
    share, iface = schur_blocks.shape[1:]
    rows = 2 * share + columns
    blocks = iface // share
    f32, dma = jnp.float32, pltpu.SemaphoreType.DMA
    vmem = pl.BlockSpec(memory_space=pltpu.VMEM)
    hbm = pl.BlockSpec(memory_space=pl.ANY)
    pairs = len(PAIRS)
    both = pl.pallas_call(
        kernel,
        out_shape=jax.ShapeDtypeStruct((2, piece, 128), f32),
        in_specs=[hbm, hbm, hbm, pl.BlockSpec(memory_space=pltpu.SMEM), hbm, hbm],
        out_specs=vmem,
        scratch_shapes=[
            pltpu.VMEM((slots, piece, columns), f32),
            pltpu.VMEM((2, share, iface), f32),
            pltpu.VMEM((slots // 4, rows, 512), jnp.bfloat16),
            pltpu.VMEM((ITERS, 2, slots, piece // 2, 128), f32),
            pltpu.VMEM((2, rows, 128), f32),
            pltpu.VMEM((ITERS, 2, slots, piece // 2, 128), f32),
            pltpu.VMEM((ITERS, 2, pairs, piece // 2, 128), f32),
            pltpu.VMEM((ITERS, 2, blocks, 2, 128), f32),
            pltpu.VMEM((ITERS, 2, blocks, 2, 128), f32),
            pltpu.VMEM((1, iface), jnp.int32),
            pltpu.VMEM((1, piece), f32),
            pltpu.VMEM((1, piece, 128), f32),
            pltpu.VMEM((blocks, 128), jnp.int32),
            pltpu.VMEM((blocks, 128), jnp.int32),
            pltpu.VMEM((2 * piece, 128), jnp.bfloat16),
            pltpu.VMEM((piece // 2, 128), f32),
            pltpu.VMEM((2, piece // 2, 128), f32),
            pltpu.VMEM((2, piece // 2, 128), f32),
            dma((slots + 4,)),
            dma(()),
            dma(()),
            dma((ITERS, 2)),
            dma((ITERS, 2, slots - 1)),
            dma((ITERS, 2)),
            dma((ITERS, 2)),
            dma((ITERS, 2)),
            dma((ITERS, 2)),
        ],
        name="sweeps",
        compiler_params=pltpu.CompilerParams(collective_id=0, has_side_effects=True),
    )(boundary_block, schur_blocks, interface_rows, live_rows, row_scale, excitation)
    return both[0:1], both[1:2]


def solution(mesh):
    placed = (
        P(None, ("narrow", "grp"), "wide"),
        P("narrow", ("wide", "grp"), None),
        P("narrow", None),
        P("narrow"),
        P("wide", ("narrow", "grp")),
        P("wide", ("narrow", "grp"), None),
    )
    return jax.shard_map(
        on_device,
        mesh=mesh,
        in_specs=placed,
        out_specs=(P("wide", ("narrow", "grp"), None), P("wide", ("narrow", "grp"), None)),
        check_vma=False,
    )
```
